32 devices in a mesh: grp: 4 (over z), hap: 8 (over y, x, core).
Axes of the slice: x: 2, y: 2, z: 4, core: 2. Of those that a mesh axis runs over, the one named last changes fastest.
Arguments:
- alleles: int32 [60, 512], P('grp', 'hap'), may hold values from 0 to 1073741823
- observed: int32 [60, 32], P('grp', 'hap'), may hold values from 0 to 2
- map_steps: int32 [60], P('grp'), may hold values from 1 to 99
- start_weights: float32 [32, 15360], P('hap'), may hold values from 1e-12 to 1
- end_weights: float32 [32, 15360], P('hap'), may hold values from 1e-12 to 1
Outputs:
- dosage: float32 [60, 32], P('grp', 'hap')
The draws below stay inside these ranges and needn't reach their ends.
Inputs may be any that keep to these rules, and one draw needn't show every extreme that they name: Bit b of alleles[m, w] is the allele 0 or 1 of reference haplotype 30 w + b at marker m. 0 and 1 are observed alleles, 2 marks a marker not typed in that target.
All inputs are finite; a program needn't handle non-finite values.
Results may differ from the reference program's by a relative error of at most 0.0008.
Values sent between devices are 32-bit elements; how exact they have to be, the bound alone decides.
A program may use at most 128 MiB of HBM per device.

```python
import math
import jax
import jax.numpy as jnp
from jax import lax

K = 15360
TGT_DEV = 4
WORDS = 512
MARKERS = 60
TARGETS = 32


def place_ends(entries, own_key, smallest, top_value):
    spot = [jax.random.randint(jax.random.fold_in(own_key, axis), (), 0, length) for axis, length in enumerate(entries.shape)]
    longest = entries.shape.index(max(entries.shape))
    next_to = spot[:longest] + [(spot[longest] + 1) % entries.shape[longest]] + spot[longest + 1:]
    return entries.at[tuple(spot)].set(smallest).at[tuple(next_to)].set(top_value)


def block_levels(rng, extent, pieces, smallest, top_value):
    level = 1.0
    for axis_at, parts in pieces:
        heights = jax.random.uniform(jax.random.fold_in(jax.random.fold_in(rng, 6), axis_at), (parts,), jnp.float32, smallest / len(pieces), top_value / len(pieces))
        level = level * jnp.repeat(jnp.exp(heights), extent[axis_at] // parts).reshape((-1,) + (1,) * (len(extent) - 1 - axis_at))
    return level


def setup_inputs(seed: int = 0) -> dict:
    key_of = jax.random.split(jax.random.key(seed), 6)
    return {
        "alleles": place_ends(jax.random.randint(key_of[0], (MARKERS, WORDS), 0, 1073741824), jax.random.fold_in(key_of[0], 1), 0, 1073741823).astype(jnp.int32),
        "observed": place_ends(jax.random.randint(key_of[1], (MARKERS, TARGETS), 0, 3), jax.random.fold_in(key_of[1], 1), 0, 2).astype(jnp.int32),
        "map_steps": place_ends(jax.random.randint(key_of[2], (MARKERS,), 1, 100), jax.random.fold_in(key_of[2], 1), 1, 99).astype(jnp.int32),
        "start_weights": jnp.clip(jnp.exp(math.log(1.0) - 27.631021 * jax.random.uniform(key_of[3], (TARGETS, K), jnp.float32) ** block_levels(key_of[3], (TARGETS, K), ((0, 8),), -0.2, 0.2)), 9.999999960041972e-13, 1.0),
        "end_weights": jnp.clip(jnp.exp(math.log(1.0) - 27.631021 * jax.random.uniform(key_of[4], (TARGETS, K), jnp.float32) ** block_levels(key_of[4], (TARGETS, K), ((0, 8),), -0.2, 0.2)), 9.999999960041972e-13, 1.0),
    }


error_rate = 0.01
map_unit = 100000.0


def unpack_alleles(packed):
    shifts = jnp.arange(30, dtype=jnp.int32)
    bits = jnp.bitwise_and(jnp.right_shift(packed[:, :, None], shifts[None, None, :]), 1)
    return bits.reshape(packed.shape[0], packed.shape[1] * 30).astype(jnp.float32)


def emission(allele_row, observed_col):
    missing = (observed_col == 2).astype(jnp.float32)[:, None]
    called = observed_col.astype(jnp.float32)[:, None]
    agree = allele_row[None, :] * called + (1.0 - allele_row[None, :]) * (1.0 - called)
    return missing + (1.0 - missing) * (error_rate + (1.0 - 2.0 * error_rate) * agree)


def forward_pass(state, haplos, observed, rates):
    total_haps = haplos.shape[1]

    def advance(carry, inputs):
        allele_row, observed_col, rate = inputs
        mixed = (1.0 - rate) * carry + (rate / total_haps) * jnp.sum(carry, axis=1, keepdims=True)
        weighted = emission(allele_row, observed_col) * mixed
        weighted = weighted / jnp.sum(weighted, axis=1, keepdims=True)
        return weighted, weighted.astype(jnp.bfloat16)

    return lax.scan(advance, state, (haplos, observed, rates))


def backward_pass(state, haplos, observed, rates):
    total_haps = haplos.shape[1]

    def retreat(carry, inputs):
        allele_row, observed_col, rate = inputs
        kept = carry.astype(jnp.bfloat16)
        weighted = emission(allele_row, observed_col) * carry
        mixed = (1.0 - rate) * weighted + (rate / total_haps) * jnp.sum(weighted, axis=1, keepdims=True)
        mixed = mixed / jnp.sum(mixed, axis=1, keepdims=True)
        return mixed, kept

    return lax.scan(retreat, state, (haplos, observed, rates), reverse=True)


def reference(alleles, observed, map_steps, start_weights, end_weights):
    haplos = unpack_alleles(alleles)
    rates = 1.0 - jnp.exp(-map_steps.astype(jnp.float32) / map_unit)
    start_rows = start_weights / jnp.sum(start_weights, axis=1, keepdims=True)
    end_rows = end_weights / jnp.sum(end_weights, axis=1, keepdims=True)
    blocks = TARGETS // TGT_DEV
    observed_blocks = observed.reshape(MARKERS, blocks, TGT_DEV).transpose(1, 0, 2)
    start_blocks = start_rows.reshape(blocks, TGT_DEV, K)
    end_blocks = end_rows.reshape(blocks, TGT_DEV, K)
    allele_half = haplos.astype(jnp.bfloat16)

    def one_block(operands):
        observed_block, start_block, end_block = operands
        _, forward_store = forward_pass(start_block, haplos, observed_block, rates)
        _, backward_store = backward_pass(end_block, haplos, observed_block, rates)
        forward_store = lax.optimization_barrier(forward_store)
        backward_store = lax.optimization_barrier(backward_store)
        carrying = backward_store * allele_half[:, None, :]
        forward_wide = forward_store.astype(jnp.float32)
        numer = jnp.einsum("mtk,mtk->mt", forward_wide, carrying.astype(jnp.float32))
        denom = jnp.einsum("mtk,mtk->mt", forward_wide, backward_store.astype(jnp.float32))
        return numer / denom

    dosage = lax.map(one_block, (observed_blocks, start_blocks, end_blocks))
    return dosage.transpose(1, 0, 2).reshape(MARKERS, TARGETS)
```

```python
import functools
import jax
import jax.numpy as jnp
from jax import lax
from jax.experimental import pallas as pl
from jax.experimental.pallas import tpu as pltpu
from jax.sharding import PartitionSpec as P

error_rate = 0.01
map_unit = 100000.0
SUB, LANE = 8, 128
MESH = pl.DeviceIdType.MESH


def total(parts):
    parts = list(parts)
    while len(parts) > 1:
        parts = [a + b for a, b in zip(parts[::2], parts[1::2])] + parts[len(parts) // 2 * 2:]
    return parts[0]


def whole_sum(parts):
    return jnp.sum(total(parts), keepdims=True)


def kernel(dims, alleles, observed, steps, starts, ends, out, tmp, meta, sbuf, recv, recv_meta,
           bits, table, staged, fstore, bstore, numer, denom, dos, out_recv,
           send_sem, recv_sem, meta_send, meta_recv, out_send, out_recv_sem):
    groups, haps, local_m, targets, words, bits_word = dims
    total_haps = words * bits_word
    local_w = words // haps
    span = words // SUB
    reps = LANE // span
    vecs = bits_word // reps
    pack = LANE // local_w
    rows = -(-local_m // pack)
    slots = pack * rows
    share = haps // SUB
    half = groups // 2
    g_me, h_me = lax.axis_index("grp"), lax.axis_index("hap")
    devices = groups * haps
    me = g_me * haps + h_me
    mine = lax.rem(g_me, targets)

    barrier = pltpu.get_barrier_semaphore()

    @pl.loop(1, devices)
    def _(d):
        peer = lax.rem(me + d, devices)
        pl.semaphore_signal(barrier, inc=1, device_id=(peer // haps, lax.rem(peer, haps)), device_id_type=MESH)

    lane = lax.broadcasted_iota(jnp.int32, (SUB, LANE), 1)
    tmp[...] = jnp.zeros_like(tmp)
    tmp[0:local_m, 0:local_w] = alleles[...]
    dense = tmp[0:SUB, :]
    for p in range(1, pack):
        dense = jnp.where(lane // local_w == p, pltpu.roll(tmp[p * rows:p * rows + SUB, :], p * local_w, 1), dense)
    sbuf[...] = dense
    recv[g_me, pl.ds(pl.multiple_of(h_me * SUB, SUB), SUB), :] = dense
    meta[...] = jnp.zeros_like(meta)
    meta[0:local_m, 0:targets] = observed[...]
    row16 = lax.broadcasted_iota(jnp.int32, meta.shape, 0)
    lane16 = lax.broadcasted_iota(jnp.int32, meta.shape, 1)
    column = meta[...]
    for i in range(local_m):
        column = jnp.where((row16 == i) & (lane16 == targets), steps[i], column)
    meta[...] = column
    recv_meta[g_me] = column

    pl.semaphore_wait(barrier, devices - 1)

    def block_copy(g, h, sem_g, sem_h):
        return pltpu.make_async_remote_copy(
            src_ref=sbuf, dst_ref=recv.at[sem_g, pl.ds(pl.multiple_of(sem_h * SUB, SUB), SUB), :],
            send_sem=send_sem.at[g, h], recv_sem=recv_sem.at[sem_g, sem_h],
            device_id=(g, h), device_id_type=MESH)

    def meta_copy(g, sem_g):
        return pltpu.make_async_remote_copy(
            src_ref=meta, dst_ref=recv_meta.at[sem_g], send_sem=meta_send.at[g], recv_sem=meta_recv.at[sem_g],
            device_id=(g, h_me), device_id_type=MESH)

    @pl.loop(1, groups)
    def _(d):
        g = lax.rem(g_me + d, groups)
        meta_copy(g, g_me).start()

    @pl.loop(1, devices)
    def _(d):
        peer = lax.rem(me + d, devices)
        block_copy(peer // haps, lax.rem(peer, haps), g_me, h_me).start()

    def arrange(weights):
        for r in range(vecs):
            for s in range(SUB):
                at = s * vecs + r
                staged[at * targets:(at + 1) * targets, :] = weights[:, at * LANE:(at + 1) * LANE]
        source = [staged[pl.ds(r * targets + mine, SUB, stride=vecs * targets), :] for r in range(vecs)]
        result = []
        for q in range(vecs):
            spot = bits_word * (lane % span) + reps * q + lane // span
            chosen, within = spot // LANE, spot % LANE
            value = jnp.zeros((SUB, LANE), jnp.float32)
            for r in range(vecs):
                moved = jnp.take_along_axis(source[r], within, axis=1, mode="promise_in_bounds")
                value = jnp.where(chosen == r, moved, value)
            result.append(value)
        inverse = 1.0 / whole_sum(result)
        return [value * inverse for value in result]

    fwd = arrange(starts)
    bwd = arrange(ends)

    @pl.loop(1, groups)
    def _(d):
        meta_copy(g_me, lax.rem(g_me + d, groups)).wait_recv()

    @pl.loop(0, groups)
    def _(g):
        entry = recv_meta[g].astype(jnp.float32)
        seen = jnp.sum(jnp.where(lane16 == mine, entry, 0.0), axis=1, keepdims=True)
        dist = jnp.sum(jnp.where(lane16 == targets, entry, 0.0), axis=1, keepdims=True)
        seen = jnp.broadcast_to(seen, entry.shape)
        dist = jnp.broadcast_to(dist, entry.shape)
        rate = 1.0 - jnp.exp(-dist / map_unit)
        at = pl.ds(pl.multiple_of(g * slots, SUB), slots)
        table[0, at, :] = jnp.where(seen == 2.0, 1.0, jnp.where(seen == 1.0, 1.0 - error_rate, error_rate))
        table[1, at, :] = jnp.where(seen == 2.0, 1.0, jnp.where(seen == 0.0, 1.0 - error_rate, error_rate))
        table[2, at, :] = 1.0 - rate
        table[3, at, :] = rate / total_haps

    def expand(g):
        @pl.loop(0, haps)
        def _(h):
            @pl.when((g != g_me) | (h != h_me))
            def _():
                block_copy(g_me, h_me, g, h).wait_recv()

        for r in range(rows):
            loads = [recv[g, pl.ds(j * SUB + r, SUB, stride=SUB * share), :] for j in range(share)]
            for p in range(pack):
                value = jnp.zeros((SUB, LANE), jnp.int32)
                for e in range(reps):
                    for j in range(share):
                        begin = e * span + j * local_w
                        shift = (begin - p * local_w) % LANE
                        piece = loads[j] if shift == 0 else pltpu.roll(loads[j], shift, 1)
                        piece = piece if e == 0 else jnp.right_shift(piece, e)
                        value = jnp.where((lane >= begin) & (lane < begin + local_w), piece, value)
                bits[g * slots + p * rows + r] = value

    def row(kind, slot):
        return jnp.broadcast_to(table[kind, pl.ds(slot, 1), :], (SUB, LANE))

    def emitted(slot):
        word = bits[slot]
        one, zero = row(0, slot), row(1, slot)
        return [jnp.where(jnp.bitwise_and(word, 1 << (reps * q)) != 0, one, zero) for q in range(vecs)]

    def rounded(values):
        return [value.astype(jnp.bfloat16).astype(jnp.float32) for value in values]

    def move_forward(f, slot):
        keep, add = row(2, slot), row(3, slot)
        w = [e * (keep * v + add) for e, v in zip(emitted(slot), f)]
        inverse = 1.0 / whole_sum(w)
        return [v * inverse for v in w]

    def move_backward(b, slot):
        w = [e * v for e, v in zip(emitted(slot), b)]
        keep, add = row(2, slot) / whole_sum(w), row(3, slot)
        return [keep * v + add for v in w]

    def store_section(s, carry):
        expand(s)
        expand(groups - 1 - s)

        def step(i, carry):
            f, b = list(carry[:vecs]), list(carry[vecs:])
            fs, bs = s * slots + i, (groups - 1 - s) * slots + local_m - 1 - i
            f = move_forward(f, fs)
            for q in range(vecs):
                fstore[s * local_m + i, q] = f[q]
                bstore[s * local_m + i, q] = b[q]
            b = move_backward(b, bs)
            return tuple(f) + tuple(b)

        return lax.fori_loop(0, local_m, step, carry)

    def score(f, b, slot):
        word = bits[slot]
        prod = [x * y for x, y in zip(rounded(f), rounded(b))]
        numer[slot] = total([jnp.where(jnp.bitwise_and(word, 1 << (reps * q)) != 0, v, 0.0) for q, v in enumerate(prod)])
        denom[slot] = total(prod)

    def score_section(s, carry):
        def step(i, carry):
            f, b = list(carry[:vecs]), list(carry[vecs:])
            fs, bs = s * slots + i, (groups - 1 - s) * slots + local_m - 1 - i
            other = (groups - 1 - s) * local_m + local_m - 1 - i
            score([fstore[other, q] for q in range(vecs)], b, bs)
            f = move_forward(f, fs)
            score(f, [bstore[other, q] for q in range(vecs)], fs)
            b = move_backward(b, bs)
            return tuple(f) + tuple(b)

        return lax.fori_loop(0, local_m, step, carry)

    carry = lax.fori_loop(0, half, store_section, tuple(fwd) + tuple(bwd))
    lax.fori_loop(half, groups, score_section, carry)

    def out_copy(g, owner):
        return pltpu.make_async_remote_copy(
            src_ref=dos.at[g], dst_ref=out_recv.at[owner], send_sem=out_send.at[g],
            recv_sem=out_recv_sem.at[owner], device_id=(g, h_me), device_id_type=MESH)

    owner = g_me < targets

    @pl.loop(0, groups)
    def _(g):
        at = pl.ds(g * slots, local_m)
        top = jnp.sum(jnp.sum(numer[at], axis=1), axis=1, keepdims=True)
        low = jnp.sum(jnp.sum(denom[at], axis=1), axis=1, keepdims=True)
        dos[g, 0:local_m, :] = jnp.broadcast_to(top / low, (local_m, LANE))

        @pl.when((g != g_me) & owner)
        def _():
            out_copy(g, g_me).start()

    @pl.when(owner)
    def _():
        out_recv[g_me, 0:local_m, :] = dos[g_me, 0:local_m, :]

    @pl.loop(0, targets)
    def _(t):
        @pl.when(t != g_me)
        def _():
            out_copy(g_me, t).wait_recv()

    lane_m = lax.broadcasted_iota(jnp.int32, (local_m, LANE), 1)
    result = jnp.zeros((local_m, LANE), jnp.float32)
    for t in range(targets):
        result = jnp.where(lane_m == t, out_recv[t, 0:local_m, :], result)
    out[...] = result[:, 0:targets]

    @pl.loop(1, groups)
    def _(d):
        g = lax.rem(g_me + d, groups)
        meta_copy(g, g_me).wait_send()

        @pl.when(owner)
        def _():
            out_copy(g, g_me).wait_send()

    @pl.loop(1, devices)
    def _(d):
        peer = lax.rem(me + d, devices)
        block_copy(peer // haps, lax.rem(peer, haps), g_me, h_me).wait_send()


def solution(mesh):
    groups, haps = mesh.shape["grp"], mesh.shape["hap"]

    def local(alleles, observed, map_steps, start_weights, end_weights):
        local_m, local_w = alleles.shape
        targets, total_haps = start_weights.shape
        words = local_w * haps
        bits_word = total_haps // words
        reps = LANE * SUB // words
        vecs = bits_word // reps
        pack = LANE // local_w
        slots = pack * -(-local_m // pack)
        markers = local_m * groups
        assert targets <= groups and groups % 2 == 0 and slots % SUB == 0
        vmem = pl.BlockSpec(memory_space=pltpu.VMEM)
        dims = (groups, haps, local_m, targets, words, bits_word)
        f32, i32 = jnp.float32, jnp.int32
        dma = pltpu.SemaphoreType.DMA
        return pl.pallas_call(
            functools.partial(kernel, dims),
            out_shape=jax.ShapeDtypeStruct((local_m, targets), f32),
            in_specs=[vmem, vmem, pl.BlockSpec(memory_space=pltpu.SMEM), vmem, vmem],
            out_specs=vmem,
            scratch_shapes=[
                pltpu.VMEM((slots + SUB, LANE), i32),
                pltpu.VMEM((slots, LANE), i32),
                pltpu.VMEM((SUB, LANE), i32),
                pltpu.VMEM((groups, haps * SUB, LANE), i32),
                pltpu.VMEM((groups, slots, LANE), i32),
                pltpu.VMEM((groups * slots, SUB, LANE), i32),
                pltpu.VMEM((4, groups * slots, LANE), f32),
                pltpu.VMEM((vecs * SUB * targets, LANE), f32),
                pltpu.VMEM((markers // 2, vecs, SUB, LANE), f32),
                pltpu.VMEM((markers // 2, vecs, SUB, LANE), f32),
                pltpu.VMEM((groups * slots, SUB, LANE), f32),
                pltpu.VMEM((groups * slots, SUB, LANE), f32),
                pltpu.VMEM((groups, slots, LANE), f32),
                pltpu.VMEM((targets, slots, LANE), f32),
                dma((groups, haps)), dma((groups, haps)),
                dma((groups,)), dma((groups,)), dma((groups,)), dma((targets,)),
            ],
            compiler_params=pltpu.CompilerParams(
                collective_id=0, has_side_effects=True, vmem_limit_bytes=48 * 1024 * 1024),
        )(alleles, observed, map_steps, start_weights, end_weights)

    in_specs = (P("grp", "hap"), P("grp", "hap"), P("grp"), P("hap", None), P("hap", None))
    return jax.shard_map(local, mesh=mesh, in_specs=in_specs, out_specs=P("grp", "hap"), check_vma=False)
```

```python
import functools
import jax
import jax.numpy as jnp
from jax import lax
from jax.experimental import pallas as pl
from jax.experimental.pallas import tpu as pltpu
from jax.sharding import PartitionSpec as P

error_rate = 0.01
map_unit = 100000.0
SUB, LANE = 8, 128
MESH = pl.DeviceIdType.MESH


def total(parts):
    parts = list(parts)
    while len(parts) > 1:
        parts = [a + b for a, b in zip(parts[::2], parts[1::2])] + parts[len(parts) // 2 * 2:]
    return parts[0]


def block_size(local_m):
    return next(n for n in (5, 4, 3, 2, 1) if local_m % n == 0)


def whole_sum(parts):
    return jnp.sum(total(parts), keepdims=True)


def kernel(dims, alleles, observed, steps, starts, ends, out, tmp, meta, sbuf, recv, recv_meta,
           bits, table, staged, fstore, bstore, emit, runs, numer, denom, dos, out_recv,
           send_sem, recv_sem, meta_send, meta_recv, out_send, out_recv_sem):
    groups, haps, local_m, targets, words, bits_word = dims
    total_haps = words * bits_word
    local_w = words // haps
    span = words // SUB
    reps = LANE // span
    vecs = bits_word // reps
    pack = LANE // local_w
    rows = -(-local_m // pack)
    slots = pack * rows
    share = haps // SUB
    half = groups // 2
    size = block_size(local_m)
    g_me, h_me = lax.axis_index("grp"), lax.axis_index("hap")
    devices = groups * haps
    me = g_me * haps + h_me
    mine = lax.rem(g_me, targets)

    barrier = pltpu.get_barrier_semaphore()

    @pl.loop(1, devices)
    def _(d):
        peer = lax.rem(me + d, devices)
        pl.semaphore_signal(barrier, inc=1, device_id=(peer // haps, lax.rem(peer, haps)), device_id_type=MESH)

    lane = lax.broadcasted_iota(jnp.int32, (SUB, LANE), 1)
    tmp[...] = jnp.zeros_like(tmp)
    tmp[0:local_m, 0:local_w] = alleles[...]
    dense = tmp[0:SUB, :]
    for p in range(1, pack):
        dense = jnp.where(lane // local_w == p, pltpu.roll(tmp[p * rows:p * rows + SUB, :], p * local_w, 1), dense)
    sbuf[...] = dense
    recv[g_me, pl.ds(pl.multiple_of(h_me * SUB, SUB), SUB), :] = dense
    meta[...] = jnp.zeros_like(meta)
    meta[0:local_m, 0:targets] = observed[...]
    row16 = lax.broadcasted_iota(jnp.int32, meta.shape, 0)
    lane16 = lax.broadcasted_iota(jnp.int32, meta.shape, 1)
    column = meta[...]
    for i in range(local_m):
        column = jnp.where((row16 == i) & (lane16 == targets), steps[i], column)
    meta[...] = column
    recv_meta[g_me] = column

    def arrange(weights):
        for r in range(vecs):
            for s in range(SUB):
                at = s * vecs + r
                staged[at * targets:(at + 1) * targets, :] = weights[:, at * LANE:(at + 1) * LANE]
        source = [staged[pl.ds(r * targets + mine, SUB, stride=vecs * targets), :] for r in range(vecs)]
        result = []
        for q in range(vecs):
            spot = bits_word * (lane % span) + reps * q + lane // span
            chosen, within = spot // LANE, spot % LANE
            value = jnp.zeros((SUB, LANE), jnp.float32)
            for r in range(vecs):
                moved = jnp.take_along_axis(source[r], within, axis=1, mode="promise_in_bounds")
                value = jnp.where(chosen == r, moved, value)
            result.append(value)
        inverse = 1.0 / whole_sum(result)
        return [value * inverse for value in result]

    fwd = arrange(starts)

    pl.semaphore_wait(barrier, devices - 1)

    def block_copy(g, h, sem_g, sem_h):
        return pltpu.make_async_remote_copy(
            src_ref=sbuf, dst_ref=recv.at[sem_g, pl.ds(pl.multiple_of(sem_h * SUB, SUB), SUB), :],
            send_sem=send_sem.at[g, h], recv_sem=recv_sem.at[sem_g, sem_h],
            device_id=(g, h), device_id_type=MESH)

    def meta_copy(g, sem_g):
        return pltpu.make_async_remote_copy(
            src_ref=meta, dst_ref=recv_meta.at[sem_g], send_sem=meta_send.at[g], recv_sem=meta_recv.at[sem_g],
            device_id=(g, h_me), device_id_type=MESH)

    @pl.loop(1, groups)
    def _(d):
        g = lax.rem(g_me + d, groups)
        meta_copy(g, g_me).start()

    @pl.loop(1, devices)
    def _(d):
        peer = lax.rem(me + d, devices)
        block_copy(peer // haps, lax.rem(peer, haps), g_me, h_me).start()

    bwd = arrange(ends)

    @pl.loop(1, groups)
    def _(d):
        meta_copy(g_me, lax.rem(g_me + d, groups)).wait_recv()

    @pl.loop(0, groups)
    def _(g):
        entry = recv_meta[g].astype(jnp.float32)
        seen = jnp.sum(jnp.where(lane16 == mine, entry, 0.0), axis=1, keepdims=True)
        dist = jnp.sum(jnp.where(lane16 == targets, entry, 0.0), axis=1, keepdims=True)
        seen = jnp.broadcast_to(seen, entry.shape)
        dist = jnp.broadcast_to(dist, entry.shape)
        rate = 1.0 - jnp.exp(-dist / map_unit)
        at = pl.ds(pl.multiple_of(g * slots, SUB), slots)
        table[0, at, :] = jnp.where(seen == 2.0, 1.0, jnp.where(seen == 1.0, 1.0 - error_rate, error_rate))
        table[1, at, :] = jnp.where(seen == 2.0, 1.0, jnp.where(seen == 0.0, 1.0 - error_rate, error_rate))
        table[2, at, :] = 1.0 - rate
        table[3, at, :] = rate / total_haps

    def expand(g):
        @pl.loop(0, haps)
        def _(h):
            @pl.when((g != g_me) | (h != h_me))
            def _():
                block_copy(g_me, h_me, g, h).wait_recv()

        for r in range(rows):
            loads = [recv[g, pl.ds(j * SUB + r, SUB, stride=SUB * share), :] for j in range(share)]
            for p in range(pack):
                value = jnp.zeros((SUB, LANE), jnp.int32)
                for e in range(reps):
                    for j in range(share):
                        begin = e * span + j * local_w
                        shift = (begin - p * local_w) % LANE
                        piece = loads[j] if shift == 0 else pltpu.roll(loads[j], shift, 1)
                        piece = piece if e == 0 else jnp.right_shift(piece, e)
                        value = jnp.where((lane >= begin) & (lane < begin + local_w), piece, value)
                bits[g * slots + p * rows + r] = value

    def row(kind, slot):
        return jnp.broadcast_to(table[kind, pl.ds(slot, 1), :], (SUB, LANE))

    def add_up(value):
        return jnp.broadcast_to(jnp.sum(value, keepdims=True), (SUB, LANE))

    pairs = [(j, i) for j in range(size) for i in range(j, size)]

    def spans(slot, block):
        sums = {pair: [] for pair in pairs}
        words_in = [bits[slot + i] for i in range(size)]
        tops = [(row(0, slot + i), row(1, slot + i)) for i in range(size)]
        for q in range(vecs):
            e = [jnp.where(jnp.bitwise_and(words_in[i], 1 << (reps * q)) != 0, *tops[i]) for i in range(size)]
            for i in range(size):
                emit[slot + i, q] = e[i]
            for j in range(size):
                run = e[j]
                for i in range(j, size):
                    run = run if i == j else run * e[i]
                    sums[j, i] = [run] if q == 0 else [sums[j, i][0] + run]
        result = {}
        for at, pair in enumerate(pairs):
            result[pair] = add_up(sums[pair][0])
            runs[block, at] = result[pair]
        return result

    def kept_spans(block):
        return {pair: runs[block, at] for at, pair in enumerate(pairs)}

    def ahead(state, order):
        sums = [None] * size
        for q in range(vecs):
            value = state[q]
            for i, slot in enumerate(order):
                value = value * emit[slot, q]
                sums[i] = value if q == 0 else sums[i] + value
        return [add_up(value) for value in sums]

    def solve_forward(first, span, order):
        keep = [row(2, slot) for slot in order]
        add = [row(3, slot) for slot in order]
        sums, terms = [], []
        lead = None
        for i in range(size):
            lead = keep[i] if i == 0 else lead * keep[i]
            terms = [term * keep[i] for term in terms]
            terms.append(add[i] if i == 0 else add[i] * sums[i - 1])
            value = lead * first[i]
            for j, term in enumerate(terms):
                value = value + term * span[j, i]
            sums.append(value)
        scale = [(1.0 if i == 0 else sums[i - 1]) / sums[i] for i in range(size)]
        return [keep[i] * scale[i] for i in range(size)], [add[i] * scale[i] for i in range(size)]

    def solve_backward(first, span, order):
        keep = [row(2, slot) for slot in order]
        add = [row(3, slot) for slot in order]
        sums, terms = [], []
        lead = None
        for i in range(size):
            value = first[i] if i == 0 else lead * first[i]
            for j, term in enumerate(terms):
                value = value + term * span[size - 1 - i, size - 2 - j]
            sums.append(value)
            lead = keep[i] if i == 0 else lead * keep[i]
            terms = [term * keep[i] for term in terms] + [add[i] * value]
        scale = [(1.0 if i == 0 else sums[i - 1]) / sums[i] for i in range(size)]
        return [keep[i] * scale[i] for i in range(size)], add

    blocks = local_m // size

    def place(s, n):
        slot = s * slots + n * size
        return slot, s * local_m + n * size, s * blocks + n

    def store_section(s, carry):
        expand(s)
        expand(groups - 1 - s)

        def step(n, carry):
            f, b = list(carry[:vecs]), list(carry[vecs:])
            fs, fm, fb = place(s, n)
            bs, _, bb = place(groups - 1 - s, blocks - 1 - n)
            bm = s * local_m + n * size
            f_order = [fs + i for i in range(size)]
            b_order = [bs + size - 1 - i for i in range(size)]
            f_span, b_span = spans(fs, fb), spans(bs, bb)
            f_first, b_first = ahead(f, f_order), ahead(b, b_order)
            f_keep, f_add = solve_forward(f_first, f_span, f_order)
            b_keep, b_add = solve_backward(b_first, b_span, b_order)
            for q in range(vecs):
                for i in range(size):
                    f[q] = emit[f_order[i], q] * (f_keep[i] * f[q] + f_add[i])
                    fstore[fm + i, q] = f[q]
                    bstore[bm + i, q] = b[q]
                    b[q] = b_keep[i] * (emit[b_order[i], q] * b[q]) + b_add[i]
            return tuple(f) + tuple(b)

        return lax.fori_loop(0, blocks, step, carry)

    def half_type(value):
        return value.astype(jnp.bfloat16).astype(jnp.float32)

    def score_section(s, carry):
        def step(n, carry):
            f, b = list(carry[:vecs]), list(carry[vecs:])
            fs, _, fb = place(s, n)
            bs, _, bb = place(groups - 1 - s, blocks - 1 - n)
            other = (groups - 1 - s) * local_m + local_m - 1 - n * size
            f_order = [fs + i for i in range(size)]
            b_order = [bs + size - 1 - i for i in range(size)]
            f_first, b_first = ahead(f, f_order), ahead(b, b_order)
            f_keep, f_add = solve_forward(f_first, kept_spans(fb), f_order)
            b_keep, b_add = solve_backward(b_first, kept_spans(bb), b_order)
            tops, lows = {}, {}

            def score(key, q, x, y, slot):
                prod = half_type(x) * half_type(y)
                part = jnp.where(jnp.bitwise_and(bits[slot], 1 << (reps * q)) != 0, prod, 0.0)
                tops[key] = part if q == 0 else tops[key] + part
                lows[key] = prod if q == 0 else lows[key] + prod

            for q in range(vecs):
                for i in range(size):
                    f[q] = emit[f_order[i], q] * (f_keep[i] * f[q] + f_add[i])
                    score((0, i), q, f[q], bstore[other - i, q], f_order[i])
                    score((1, i), q, fstore[other - i, q], b[q], b_order[i])
                    b[q] = b_keep[i] * (emit[b_order[i], q] * b[q]) + b_add[i]
            for i in range(size):
                numer[f_order[i]], denom[f_order[i]] = tops[0, i], lows[0, i]
                numer[b_order[i]], denom[b_order[i]] = tops[1, i], lows[1, i]
            return tuple(f) + tuple(b)

        return lax.fori_loop(0, blocks, step, carry)

    carry = lax.fori_loop(0, half, store_section, tuple(fwd) + tuple(bwd))
    lax.fori_loop(half, groups, score_section, carry)

    def out_copy(g, owner):
        return pltpu.make_async_remote_copy(
            src_ref=dos.at[g], dst_ref=out_recv.at[owner], send_sem=out_send.at[g],
            recv_sem=out_recv_sem.at[owner], device_id=(g, h_me), device_id_type=MESH)

    owner = g_me < targets

    @pl.loop(0, groups, unroll=min(groups, 4))
    def _(g):
        at = pl.ds(g * slots, local_m)
        top = jnp.sum(jnp.sum(numer[at], axis=1), axis=1, keepdims=True)
        low = jnp.sum(jnp.sum(denom[at], axis=1), axis=1, keepdims=True)
        dos[g, 0:local_m, :] = jnp.broadcast_to(top / low, (local_m, LANE))

        @pl.when((g != g_me) & owner)
        def _():
            out_copy(g, g_me).start()

    @pl.when(owner)
    def _():
        out_recv[g_me, 0:local_m, :] = dos[g_me, 0:local_m, :]

    @pl.loop(0, targets)
    def _(t):
        @pl.when(t != g_me)
        def _():
            out_copy(g_me, t).wait_recv()

    lane_m = lax.broadcasted_iota(jnp.int32, (local_m, LANE), 1)
    result = jnp.zeros((local_m, LANE), jnp.float32)
    for t in range(targets):
        result = jnp.where(lane_m == t, out_recv[t, 0:local_m, :], result)
    out[...] = result[:, 0:targets]

    @pl.loop(1, groups)
    def _(d):
        g = lax.rem(g_me + d, groups)
        meta_copy(g, g_me).wait_send()

        @pl.when(owner)
        def _():
            out_copy(g, g_me).wait_send()

    @pl.loop(1, devices)
    def _(d):
        peer = lax.rem(me + d, devices)
        block_copy(peer // haps, lax.rem(peer, haps), g_me, h_me).wait_send()


def solution(mesh):
    groups, haps = mesh.shape["grp"], mesh.shape["hap"]

    def local(alleles, observed, map_steps, start_weights, end_weights):
        local_m, local_w = alleles.shape
        targets, total_haps = start_weights.shape
        words = local_w * haps
        bits_word = total_haps // words
        reps = LANE * SUB // words
        vecs = bits_word // reps
        pack = LANE // local_w
        slots = pack * -(-local_m // pack)
        markers = local_m * groups
        size = block_size(local_m)
        assert targets <= groups and groups % 2 == 0 and slots % SUB == 0
        vmem = pl.BlockSpec(memory_space=pltpu.VMEM)
        dims = (groups, haps, local_m, targets, words, bits_word)
        f32, i32 = jnp.float32, jnp.int32
        dma = pltpu.SemaphoreType.DMA
        return pl.pallas_call(
            functools.partial(kernel, dims),
            out_shape=jax.ShapeDtypeStruct((local_m, targets), f32),
            in_specs=[vmem, vmem, pl.BlockSpec(memory_space=pltpu.SMEM), vmem, vmem],
            out_specs=vmem,
            scratch_shapes=[
                pltpu.VMEM((slots + SUB, LANE), i32),
                pltpu.VMEM((slots, LANE), i32),
                pltpu.VMEM((SUB, LANE), i32),
                pltpu.VMEM((groups, haps * SUB, LANE), i32),
                pltpu.VMEM((groups, slots, LANE), i32),
                pltpu.VMEM((groups * slots, SUB, LANE), i32),
                pltpu.VMEM((4, groups * slots, LANE), f32),
                pltpu.VMEM((vecs * SUB * targets, LANE), f32),
                pltpu.VMEM((markers // 2, vecs, SUB, LANE), f32),
                pltpu.VMEM((markers // 2, vecs, SUB, LANE), f32),
                pltpu.VMEM((groups * slots, vecs, SUB, LANE), f32),
                pltpu.VMEM((markers // size, size * (size + 1) // 2, SUB, LANE), f32),
                pltpu.VMEM((groups * slots, SUB, LANE), f32),
                pltpu.VMEM((groups * slots, SUB, LANE), f32),
                pltpu.VMEM((groups, slots, LANE), f32),
                pltpu.VMEM((targets, slots, LANE), f32),
                dma((groups, haps)), dma((groups, haps)),
                dma((groups,)), dma((groups,)), dma((groups,)), dma((targets,)),
            ],
            compiler_params=pltpu.CompilerParams(
                collective_id=0, has_side_effects=True, vmem_limit_bytes=48 * 1024 * 1024),
        )(alleles, observed, map_steps, start_weights, end_weights)

    in_specs = (P("grp", "hap"), P("grp", "hap"), P("grp"), P("hap", None), P("hap", None))
    return jax.shard_map(local, mesh=mesh, in_specs=in_specs, out_specs=P("grp", "hap"), check_vma=False)
```

```python
import functools
import jax
import jax.numpy as jnp
from jax import lax
from jax.experimental import pallas as pl
from jax.experimental.pallas import tpu as pltpu
from jax.sharding import PartitionSpec as P

error_rate = 0.01
map_unit = 100000.0
SUB, LANE = 8, 128
MESH = pl.DeviceIdType.MESH


def total(parts):
    parts = list(parts)
    while len(parts) > 1:
        parts = [a + b for a, b in zip(parts[::2], parts[1::2])] + parts[len(parts) // 2 * 2:]
    return parts[0]


def block_size(local_m):
    return next(n for n in (5, 4, 3, 2, 1) if local_m % n == 0)


def whole_sum(parts):
    return jnp.sum(total(parts), keepdims=True)


def kernel(dims, alleles, observed, steps, starts, ends, out, tmp, meta, sbuf, recv, recv_meta,
           bits, table, staged, fstore, bstore, emit, runs, numer, denom, dos, out_recv,
           start_rows, end_rows, weight_sem, send_sem, recv_sem, meta_send, meta_recv, out_send, out_recv_sem):
    groups, haps, local_m, targets, words, bits_word = dims
    total_haps = words * bits_word
    local_w = words // haps
    span = words // SUB
    reps = LANE // span
    vecs = bits_word // reps
    pack = LANE // local_w
    rows = -(-local_m // pack)
    slots = pack * rows
    share = haps // SUB
    half = groups // 2
    size = block_size(local_m)
    g_me, h_me = lax.axis_index("grp"), lax.axis_index("hap")
    devices = groups * haps
    mine = lax.rem(g_me, targets)

    weight_copies = [
        pltpu.make_async_copy(source, target, weight_sem.at[n])
        for n, (source, target) in enumerate([(starts, start_rows), (ends, end_rows)])
    ]
    for copy in weight_copies:
        copy.start()

    def each_peer(act):
        def visit(k, d):
            g = jnp.where(g_me < half, groups - 1 - k, k)
            h = lax.rem(h_me + d, haps)
            if isinstance(d, int) and d:
                act(g, h)
            else:
                pl.when((g != g_me) | (h != h_me))(lambda: act(g, h))

        if devices <= 64:
            for k in range(groups):
                for d in range(haps):
                    visit(k, d)
        else:
            @pl.loop(0, groups)
            def _(k):
                pl.loop(0, haps)(functools.partial(visit, k))

    barrier = pltpu.get_barrier_semaphore()
    each_peer(lambda g, h: pl.semaphore_signal(barrier, inc=1, device_id=(g, h), device_id_type=MESH))

    lane = lax.broadcasted_iota(jnp.int32, (SUB, LANE), 1)
    tmp[...] = jnp.zeros_like(tmp)
    tmp[0:local_m, 0:local_w] = alleles[...]
    dense = tmp[0:SUB, :]
    for p in range(1, pack):
        dense = jnp.where(lane // local_w == p, pltpu.roll(tmp[p * rows:p * rows + SUB, :], p * local_w, 1), dense)
    sbuf[...] = dense
    recv[g_me, pl.ds(pl.multiple_of(h_me * SUB, SUB), SUB), :] = dense
    meta[...] = jnp.zeros_like(meta)
    meta[0:targets, 0:local_m] = observed[...]
    columns = meta[...]
    sub_at = lax.broadcasted_iota(jnp.int32, (SUB, LANE), 0)
    for i in range(local_m):
        columns = jnp.where((sub_at == targets) & (lane == i), steps[i], columns)
    meta[...] = columns
    recv_meta[g_me] = columns

    def arrange(weights):
        for r in range(vecs):
            for s in range(SUB):
                at = s * vecs + r
                staged[at * targets:(at + 1) * targets, :] = weights[:, at * LANE:(at + 1) * LANE]
        source = [staged[pl.ds(r * targets + mine, SUB, stride=vecs * targets), :] for r in range(vecs)]
        result = []
        for q in range(vecs):
            spot = bits_word * (lane % span) + reps * q + lane // span
            chosen, within = spot // LANE, spot % LANE
            value = jnp.zeros((SUB, LANE), jnp.float32)
            for r in range(vecs):
                moved = jnp.take_along_axis(source[r], within, axis=1, mode="promise_in_bounds")
                value = jnp.where(chosen == r, moved, value)
            result.append(value)
        inverse = 1.0 / whole_sum(result)
        return [value * inverse for value in result]

    weight_copies[0].wait()
    fwd = arrange(start_rows)

    pl.semaphore_wait(barrier, devices - 1)

    def block_copy(g, h, sem_g, sem_h):
        return pltpu.make_async_remote_copy(
            src_ref=sbuf, dst_ref=recv.at[sem_g, pl.ds(pl.multiple_of(sem_h * SUB, SUB), SUB), :],
            send_sem=send_sem.at[g, h], recv_sem=recv_sem.at[sem_g, sem_h],
            device_id=(g, h), device_id_type=MESH)

    def meta_copy(g, sem_g):
        return pltpu.make_async_remote_copy(
            src_ref=meta, dst_ref=recv_meta.at[sem_g], send_sem=meta_send.at[g], recv_sem=meta_recv.at[sem_g],
            device_id=(g, h_me), device_id_type=MESH)

    @pl.loop(1, groups)
    def _(d):
        g = lax.rem(g_me + d, groups)
        meta_copy(g, g_me).start()

    def send_blocks():
        each_peer(lambda g, h: block_copy(g, h, g_me, h_me).start())

    outer = (g_me == 0) | (g_me == groups - 1)
    pl.when(outer)(send_blocks)
    weight_copies[1].wait()
    bwd = arrange(end_rows)
    pl.when(jnp.logical_not(outer))(send_blocks)

    @pl.loop(1, groups)
    def _(d):
        meta_copy(g_me, lax.rem(g_me + d, groups)).wait_recv()

    @pl.loop(0, groups)
    def _(g):
        entry = recv_meta.at[g]
        same = lax.broadcasted_iota(jnp.int32, (slots, LANE), 0) == lax.broadcasted_iota(jnp.int32, (slots, LANE), 1)

        def turned(at):
            values = jnp.broadcast_to(entry[pl.ds(at, 1), :].astype(jnp.float32), (slots, LANE))
            summed = jnp.sum(jnp.where(same, values, 0.0), axis=1, keepdims=True)
            return jnp.broadcast_to(summed, (slots, LANE))

        seen, dist = turned(mine), turned(targets)
        rate = 1.0 - jnp.exp(-dist / map_unit)
        at = pl.ds(pl.multiple_of(g * slots, SUB), slots)
        table[0, at, :] = jnp.where(seen == 2.0, 1.0, jnp.where(seen == 1.0, 1.0 - error_rate, error_rate))
        table[1, at, :] = jnp.where(seen == 2.0, 1.0, jnp.where(seen == 0.0, 1.0 - error_rate, error_rate))
        table[2, at, :] = 1.0 - rate
        table[3, at, :] = rate / total_haps

    def expand(g):
        @pl.loop(0, haps)
        def _(h):
            @pl.when((g != g_me) | (h != h_me))
            def _():
                block_copy(g_me, h_me, g, h).wait_recv()

        for r in range(rows):
            loads = [recv[g, pl.ds(j * SUB + r, SUB, stride=SUB * share), :] for j in range(share)]
            for p in range(pack):
                value = jnp.zeros((SUB, LANE), jnp.int32)
                for e in range(reps):
                    for j in range(share):
                        begin = e * span + j * local_w
                        shift = (begin - p * local_w) % LANE
                        piece = loads[j] if shift == 0 else pltpu.roll(loads[j], shift, 1)
                        piece = piece if e == 0 else jnp.right_shift(piece, e)
                        value = jnp.where((lane >= begin) & (lane < begin + local_w), piece, value)
                bits[g * slots + p * rows + r] = value

    def row(kind, slot):
        return jnp.broadcast_to(table[kind, pl.ds(slot, 1), :], (SUB, LANE))

    def add_up(value):
        for shift in (4, 2, 1):
            value = value + pltpu.roll(value, shift, 0)
        return jnp.broadcast_to(jnp.sum(value, axis=1, keepdims=True), (SUB, LANE))

    pairs = [(j, i) for j in range(size) for i in range(j, size)]

    def spans(slot, block):
        sums = {pair: [] for pair in pairs}
        words_in = [bits[slot + i] for i in range(size)]
        tops = [(row(0, slot + i), row(1, slot + i)) for i in range(size)]
        for q in range(vecs):
            e = [jnp.where(jnp.bitwise_and(words_in[i], 1 << (reps * q)) != 0, *tops[i]) for i in range(size)]
            for i in range(size):
                emit[slot + i, q] = e[i]
            for j in range(size):
                run = e[j]
                for i in range(j, size):
                    run = run if i == j else run * e[i]
                    sums[j, i] = [run] if q == 0 else [sums[j, i][0] + run]
        result = {}
        for at, pair in enumerate(pairs):
            result[pair] = add_up(sums[pair][0])
            runs[block, at] = result[pair]
        return result

    def kept_spans(block):
        return {pair: runs[block, at] for at, pair in enumerate(pairs)}

    def ahead(state, order):
        sums = [None] * size
        for q in range(vecs):
            value = state[q]
            for i, slot in enumerate(order):
                value = value * emit[slot, q]
                sums[i] = value if q == 0 else sums[i] + value
        return [add_up(value) for value in sums]

    def solve_forward(first, span, order):
        keep = [row(2, slot) for slot in order]
        add = [row(3, slot) for slot in order]
        sums, terms = [], []
        lead = None
        for i in range(size):
            lead = keep[i] if i == 0 else lead * keep[i]
            terms = [term * keep[i] for term in terms]
            terms.append(add[i] if i == 0 else add[i] * sums[i - 1])
            value = lead * first[i]
            for j, term in enumerate(terms):
                value = value + term * span[j, i]
            sums.append(value)
        scale = [(1.0 if i == 0 else sums[i - 1]) / sums[i] for i in range(size)]
        return [keep[i] * scale[i] for i in range(size)], [add[i] * scale[i] for i in range(size)]

    def solve_backward(first, span, order):
        keep = [row(2, slot) for slot in order]
        add = [row(3, slot) for slot in order]
        sums, terms = [], []
        lead = None
        for i in range(size):
            value = first[i] if i == 0 else lead * first[i]
            for j, term in enumerate(terms):
                value = value + term * span[size - 1 - i, size - 2 - j]
            sums.append(value)
            lead = keep[i] if i == 0 else lead * keep[i]
            terms = [term * keep[i] for term in terms] + [add[i] * value]
        scale = [(1.0 if i == 0 else sums[i - 1]) / sums[i] for i in range(size)]
        return [keep[i] * scale[i] for i in range(size)], add

    blocks = local_m // size

    def place(s, n):
        slot = s * slots + n * size
        return slot, s * local_m + n * size, s * blocks + n

    def store_section(s, carry):
        expand(s)
        expand(groups - 1 - s)

        def step(n, carry):
            f, b = list(carry[:vecs]), list(carry[vecs:])
            fs, fm, fb = place(s, n)
            bs, _, bb = place(groups - 1 - s, blocks - 1 - n)
            bm = s * local_m + n * size
            f_order = [fs + i for i in range(size)]
            b_order = [bs + size - 1 - i for i in range(size)]
            f_span, b_span = spans(fs, fb), spans(bs, bb)
            f_first, b_first = ahead(f, f_order), ahead(b, b_order)
            f_keep, f_add = solve_forward(f_first, f_span, f_order)
            b_keep, b_add = solve_backward(b_first, b_span, b_order)
            for q in range(vecs):
                for i in range(size):
                    f[q] = emit[f_order[i], q] * (f_keep[i] * f[q] + f_add[i])
                    fstore[fm + i, q] = f[q]
                    bstore[bm + i, q] = b[q]
                    b[q] = b_keep[i] * (emit[b_order[i], q] * b[q]) + b_add[i]
            return tuple(f) + tuple(b)

        return lax.fori_loop(0, blocks, step, carry)

    def half_type(value):
        return value.astype(jnp.bfloat16).astype(jnp.float32)

    def out_copy(g, owner):
        return pltpu.make_async_remote_copy(
            src_ref=dos.at[g], dst_ref=out_recv.at[owner], send_sem=out_send.at[g],
            recv_sem=out_recv_sem.at[owner], device_id=(g, h_me), device_id_type=MESH)

    owner = g_me < targets

    def finish(*finished):
        for g in finished:
            at = pl.ds(g * slots, local_m)
            top = jnp.sum(jnp.sum(numer[at], axis=1), axis=1, keepdims=True)
            low = jnp.sum(jnp.sum(denom[at], axis=1), axis=1, keepdims=True)
            dos[g, 0:local_m, :] = jnp.broadcast_to(top / low, (local_m, LANE))
        for g in finished:
            pl.when((g != g_me) & owner)(out_copy(g, g_me).start)

    def score_section(s, carry):
        def step(n, carry):
            f, b = list(carry[:vecs]), list(carry[vecs:])
            fs, _, fb = place(s, n)
            bs, _, bb = place(groups - 1 - s, blocks - 1 - n)
            other = (groups - 1 - s) * local_m + local_m - 1 - n * size
            f_order = [fs + i for i in range(size)]
            b_order = [bs + size - 1 - i for i in range(size)]
            f_first, b_first = ahead(f, f_order), ahead(b, b_order)
            f_keep, f_add = solve_forward(f_first, kept_spans(fb), f_order)
            b_keep, b_add = solve_backward(b_first, kept_spans(bb), b_order)
            tops, lows = {}, {}

            def score(key, q, x, y, slot):
                prod = half_type(x) * half_type(y)
                part = jnp.where(jnp.bitwise_and(bits[slot], 1 << (reps * q)) != 0, prod, 0.0)
                tops[key] = part if q == 0 else tops[key] + part
                lows[key] = prod if q == 0 else lows[key] + prod

            for q in range(vecs):
                for i in range(size):
                    f[q] = emit[f_order[i], q] * (f_keep[i] * f[q] + f_add[i])
                    score((0, i), q, f[q], bstore[other - i, q], f_order[i])
                    score((1, i), q, fstore[other - i, q], b[q], b_order[i])
                    b[q] = b_keep[i] * (emit[b_order[i], q] * b[q]) + b_add[i]
            for i in range(size):
                numer[f_order[i]], denom[f_order[i]] = tops[0, i], lows[0, i]
                numer[b_order[i]], denom[b_order[i]] = tops[1, i], lows[1, i]
            return tuple(f) + tuple(b)

        carry = lax.fori_loop(0, blocks, step, carry)
        finish(s, groups - 1 - s)
        return carry

    carry = lax.fori_loop(0, half, store_section, tuple(fwd) + tuple(bwd))
    lax.fori_loop(half, groups, score_section, carry)

    @pl.loop(1, groups)
    def _(d):
        meta_copy(lax.rem(g_me + d, groups), g_me).wait_send()

    each_peer(lambda g, h: block_copy(g, h, g_me, h_me).wait_send())

    @pl.when(owner)
    def _():
        out_recv[g_me, 0:local_m, :] = dos[g_me, 0:local_m, :]

    @pl.loop(0, targets)
    def _(t):
        @pl.when(t != g_me)
        def _():
            out_copy(g_me, t).wait_recv()

    lane_m = lax.broadcasted_iota(jnp.int32, (local_m, LANE), 1)
    result = jnp.zeros((local_m, LANE), jnp.float32)
    for t in range(targets):
        result = jnp.where(lane_m == t, out_recv[t, 0:local_m, :], result)
    out[...] = result[:, 0:targets]

    @pl.when(owner)
    def _():
        @pl.loop(1, groups)
        def _(d):
            out_copy(lax.rem(g_me + d, groups), g_me).wait_send()


def solution(mesh):
    groups, haps = mesh.shape["grp"], mesh.shape["hap"]

    def local(alleles, observed, map_steps, start_weights, end_weights):
        local_m, local_w = alleles.shape
        targets, total_haps = start_weights.shape
        words = local_w * haps
        bits_word = total_haps // words
        reps = LANE * SUB // words
        vecs = bits_word // reps
        pack = LANE // local_w
        slots = pack * -(-local_m // pack)
        markers = local_m * groups
        size = block_size(local_m)
        assert targets < SUB and targets <= groups and groups % 2 == 0 and slots % SUB == 0
        vmem = pl.BlockSpec(memory_space=pltpu.VMEM)
        dims = (groups, haps, local_m, targets, words, bits_word)
        f32, i32 = jnp.float32, jnp.int32
        dma = pltpu.SemaphoreType.DMA
        return pl.pallas_call(
            functools.partial(kernel, dims),
            out_shape=jax.ShapeDtypeStruct((local_m, targets), f32),
            in_specs=[vmem, vmem, pl.BlockSpec(memory_space=pltpu.SMEM)] + [pl.BlockSpec(memory_space=pltpu.HBM)] * 2,
            out_specs=vmem,
            scratch_shapes=[
                pltpu.VMEM((slots + SUB, LANE), i32),
                pltpu.VMEM((SUB, LANE), i32),
                pltpu.VMEM((SUB, LANE), i32),
                pltpu.VMEM((groups, haps * SUB, LANE), i32),
                pltpu.VMEM((groups, SUB, LANE), i32),
                pltpu.VMEM((groups * slots, SUB, LANE), i32),
                pltpu.VMEM((4, groups * slots, LANE), f32),
                pltpu.VMEM((vecs * SUB * targets, LANE), f32),
                pltpu.VMEM((markers // 2, vecs, SUB, LANE), f32),
                pltpu.VMEM((markers // 2, vecs, SUB, LANE), f32),
                pltpu.VMEM((groups * slots, vecs, SUB, LANE), f32),
                pltpu.VMEM((markers // size, size * (size + 1) // 2, SUB, LANE), f32),
                pltpu.VMEM((groups * slots, SUB, LANE), f32),
                pltpu.VMEM((groups * slots, SUB, LANE), f32),
                pltpu.VMEM((groups, slots, LANE), f32),
                pltpu.VMEM((targets, slots, LANE), f32),
                pltpu.VMEM((targets, total_haps), f32), pltpu.VMEM((targets, total_haps), f32), dma((2,)),
                dma((groups, haps)), dma((groups, haps)),
                dma((groups,)), dma((groups,)), dma((groups,)), dma((targets,)),
            ],
            compiler_params=pltpu.CompilerParams(
                collective_id=0, has_side_effects=True, vmem_limit_bytes=60 * 1024 * 1024),
        )(alleles, observed.T, map_steps, start_weights, end_weights)

    in_specs = (P("grp", "hap"), P("grp", "hap"), P("grp"), P("hap", None), P("hap", None))
    return jax.shard_map(local, mesh=mesh, in_specs=in_specs, out_specs=P("grp", "hap"), check_vma=False)
```
